32 devices in a mesh: row: 8 (over z, x), col: 4 (over y, core).
Axes of the slice: x: 2, y: 2, z: 4, core: 2. Of those that a mesh axis runs over, the one named last changes fastest.
Arguments:
- visible_data: bfloat16 [512, 32768], P('col', 'row'), may hold values from 0 to 1
- hidden_uniform: float32 [512, 16384], P('row', 'col'), may hold values from 0.01 to 0.99
- visible_uniform: float32 [512, 32768], P('col', 'row'), may hold values from 0.01 to 0.99
- weights: bfloat16 [32768, 16384], P('row', 'col'), may hold values from -0.03125 to 0.03125
- visible_bias: float32 [32768], P('row'), may hold values from -4 to 4
- hidden_bias: float32 [16384], P('col'), may hold values from -4 to 4
Outputs:
- grad_weights: bfloat16 [32768, 16384], P('row', 'col')
- grad_visible: float32 [32768], P('row')
- grad_hidden: float32 [16384], P('col')
- hidden_sample: bfloat16 [512, 16384], P('row', 'col')
- reconstruction: bfloat16 [512, 32768], P('col', 'row')
The draws below stay inside these ranges and needn't reach their ends.
All inputs are finite; a program needn't handle non-finite values.
Results may differ from the reference program's by a relative error of at most 0.0034.
Values may be sent and summed in bfloat16 or wider, within the bound.
A program may use at most 192 MiB of HBM per device.

```python
import jax
import jax.numpy as jnp

V = 32768
H = 16384
BATCH = 512


def block_scale(key, dims, shards, low, largest):
    gain, own = 1.0, jax.random.fold_in(key, 6)
    for dim, blocks in shards:
        draws = jnp.exp(jax.random.uniform(jax.random.fold_in(own, dim), (blocks,), jnp.float32, low / len(shards), largest / len(shards)))
        gain = gain * jnp.repeat(draws, dims[dim] // blocks).reshape([-1 if axis == dim else 1 for axis in range(len(dims))])
    return gain


def noise(rng, extent, spread, bound, cuts=(), dtype=jnp.bfloat16):
    values = jax.random.normal(rng, extent, jnp.float32) * spread
    if len(cuts) > 0:
        values = block_scale(rng, extent, cuts, -0.22, 0.18) * values
    return jnp.clip(values, min=-bound, max=bound).astype(dtype)


def setup_inputs(seed: int = 0) -> dict:
    splits = jax.random.split(jax.random.key(seed), 7)
    visible_data = jnp.clip(1.0 * jax.random.uniform(splits[0], (BATCH, V), jnp.float32) ** block_scale(splits[0], (BATCH, V), ((0, 4), (1, 8)), -0.2, 0.2), 0.0, 1.0).astype(jnp.bfloat16)
    hidden_uniform = jnp.clip(0.01 + 0.98 * jax.random.uniform(splits[1], (BATCH, H), jnp.float32) ** block_scale(splits[1], (BATCH, H), ((0, 8), (1, 4)), -0.2, 0.2), 0.01, 0.99)
    visible_uniform = jnp.clip(0.01 + 0.98 * jax.random.uniform(splits[2], (BATCH, V), jnp.float32) ** block_scale(splits[2], (BATCH, V), ((0, 4), (1, 8)), -0.2, 0.2), 0.01, 0.99)
    weights = noise(splits[3], (V, H), V ** -0.5, 0.03125, ((0, 8), (1, 4)))
    visible_bias = noise(splits[4], (V,), 1.0, 4.0, ((0, 8),), jnp.float32)
    hidden_bias = noise(splits[5], (H,), 1.0, 4.0, ((0, 4),), jnp.float32)
    return {"visible_data": visible_data, "hidden_uniform": hidden_uniform, "visible_uniform": visible_uniform, "weights": weights, "visible_bias": visible_bias, "hidden_bias": hidden_bias}


def relaxed(field, uniform):
    return jax.nn.sigmoid(2.0 * (field + jnp.log(uniform) - jnp.log1p(-uniform)))


def reference(visible_data, hidden_uniform, visible_uniform, weights, visible_bias, hidden_bias):
    field_pos = jnp.dot(visible_data, weights, preferred_element_type=jnp.float32) + hidden_bias
    probs_pos = jax.nn.sigmoid(field_pos).astype(jnp.bfloat16)
    hidden_sample = relaxed(field_pos, hidden_uniform).astype(jnp.bfloat16)
    field_neg = jnp.dot(hidden_sample, weights.T, preferred_element_type=jnp.float32) + visible_bias
    reconstruction = relaxed(field_neg, visible_uniform).astype(jnp.bfloat16)
    field_back = jnp.dot(reconstruction, weights, preferred_element_type=jnp.float32) + hidden_bias
    probs_neg = jax.nn.sigmoid(field_back).astype(jnp.bfloat16)
    positive = jnp.dot(visible_data.T, probs_pos, preferred_element_type=jnp.float32)
    negative = jnp.dot(reconstruction.T, probs_neg, preferred_element_type=jnp.float32)
    grad_weights = ((positive - negative) / BATCH).astype(jnp.bfloat16)
    grad_visible = jnp.mean(visible_data.astype(jnp.float32) - reconstruction.astype(jnp.float32), axis=0)
    grad_hidden = jnp.mean(probs_pos.astype(jnp.float32) - probs_neg.astype(jnp.float32), axis=0)
    return grad_weights, grad_visible, grad_hidden, hidden_sample, reconstruction
```

```python
import jax
import jax.numpy as jnp
from jax import lax
from jax.sharding import PartitionSpec as P


def relaxed(field, uniform):
    return jax.nn.sigmoid(2.0 * (field + jnp.log(uniform) - jnp.log1p(-uniform)))


def scatter_sum(partial_value, axis):
    narrow = partial_value.astype(jnp.bfloat16)
    return lax.psum_scatter(narrow, axis, scatter_dimension=0, tiled=True).astype(jnp.float32)


def gather(value, axis):
    return lax.all_gather(value, axis, axis=0, tiled=True)


def on_device(visible_data, hidden_uniform, visible_uniform, weights, visible_bias, hidden_bias):
    batch_total = visible_data.shape[0] * lax.axis_size("col")
    transposed = (((1,), (1,)), ((), ()))
    contract_batch = (((0,), (0,)), ((), ()))
    visible_full = gather(visible_data, "col")

    def hidden_field(source):
        partial_value = jnp.dot(source, weights, preferred_element_type=jnp.float32)
        return scatter_sum(partial_value, "row") + hidden_bias

    field_pos = hidden_field(visible_full)
    probs_pos = jax.nn.sigmoid(field_pos).astype(jnp.bfloat16)
    sample_own = relaxed(field_pos, hidden_uniform).astype(jnp.bfloat16)
    sample_full = gather(sample_own, "row")
    visible_partial = lax.dot_general(
        sample_full, weights, transposed, preferred_element_type=jnp.float32
    )
    field_neg = scatter_sum(visible_partial, "col") + visible_bias
    recon_own = relaxed(field_neg, visible_uniform).astype(jnp.bfloat16)
    recon_full = gather(recon_own, "col")
    probs_full = gather(probs_pos, "row")
    probs_back = jax.nn.sigmoid(hidden_field(recon_full)).astype(jnp.bfloat16)
    negative_full = gather(probs_back, "row")
    left_side = jnp.concatenate([visible_full, recon_full], axis=0)
    right_side = jnp.concatenate([probs_full, -negative_full], axis=0)
    difference = lax.dot_general(
        left_side, right_side, contract_batch, preferred_element_type=jnp.float32
    )
    grad_weights = (difference / batch_total).astype(jnp.bfloat16)
    grad_visible = jnp.mean(
        visible_full.astype(jnp.float32) - recon_full.astype(jnp.float32), axis=0
    )
    grad_hidden = jnp.mean(
        probs_full.astype(jnp.float32) - negative_full.astype(jnp.float32), axis=0
    )
    return (grad_weights, grad_visible, grad_hidden, sample_own, recon_own)


def solution(mesh):
    placed = (
        P("col", "row"),
        P("row", "col"),
        P("col", "row"),
        P("row", "col"),
        P("row"),
        P("col"),
    )
    return jax.shard_map(
        on_device,
        mesh=mesh,
        in_specs=placed,
        out_specs=(P("row", "col"), P("row"), P("col"), P("row", "col"), P("col", "row")),
        check_vma=False,
    )
```
